32 devices in a mesh: win: 4 (over z), step: 8 (over y, x, core).
Axes of the slice: x: 2, y: 2, z: 4, core: 2. Of those that a mesh axis runs over, the one named last changes fastest.
Arguments:
- initial_state: float32 [32, 32, 128], replicated, may hold values from -6 to 6
- source: float32 [4, 8, 32, 32, 128], P('win', 'step'), may hold values from -6 to 6
- absorption: float32 [32, 32, 128], replicated, may hold values from 0.01 to 0.2
Outputs:
- state: float32 [4, 8, 32, 32, 128], P('win', 'step')
The draws below stay inside these ranges and needn't reach their ends.
All inputs are finite; a program needn't handle non-finite values.
Results may differ from the reference program's by a relative error of at most 0.00026.
Values sent between devices are 32-bit elements; how exact they have to be, the bound alone decides.
No kernel may reach another device: no remote copies, remote signals or barrier semaphores. Data moves between devices by JAX's collectives and lax.ppermute only.
A program may use at most 64 MiB of HBM per device.

```python
import math
import jax
import jax.numpy as jnp

NX = 32
NY = 32
NZ = 128
ITERS = 2
SWEEPS = 8
STEPS = 8
WINDOWS = 4


def block_scale(rng, dims, split, low, largest):
    def one(dim, blocks):
        heights = jax.random.uniform(jax.random.fold_in(jax.random.fold_in(rng, 6), dim), (blocks,), jnp.float32, low / len(split), largest / len(split))
        return jnp.repeat(jnp.exp(heights), dims[dim] // blocks).reshape((-1,) + (1,) * (len(dims) - dim - 1))

    loudness = one(*split[0])
    for cut in split[1:]:
        loudness = loudness * one(*cut)
    return loudness


def centred(own_key, extent, spread, most, shards=(), kind=jnp.bfloat16):
    factor_of = block_scale(own_key, extent, shards, -0.22, 0.18) if shards else 1.0
    values = jax.random.normal(own_key, extent, jnp.float32) * spread * factor_of
    return jnp.minimum(jnp.maximum(values, -most), most).astype(kind)


def setup_inputs(seed: int = 0) -> dict:
    keys = jax.random.split(jax.random.key(seed), 4)
    initial_state = centred(keys[0], (NX, NY, NZ), 1.0, 6.0, (), jnp.float32)
    source = centred(keys[1], (WINDOWS, STEPS, NX, NY, NZ), 1.0, 6.0, ((0, 4), (1, 8)), jnp.float32)
    absorption = jnp.clip(jnp.exp(jax.random.uniform(keys[2], (NX, NY, NZ), jnp.float32, math.log(0.01), math.log(0.2))), 0.01, 0.2)
    return dict(initial_state=initial_state, source=source, absorption=absorption)


alpha_corner = 0.1
coupling = 0.05


def pad_cube(field):
    widths = [(0, 0)] * (field.ndim - 3) + [(1, 1)] * 3
    return jnp.pad(field, widths)


def neighbours(field):
    padded = pad_cube(field)
    total = padded[..., 2:, 1:-1, 1:-1] + padded[..., :-2, 1:-1, 1:-1]
    total = total + padded[..., 1:-1, 2:, 1:-1] + padded[..., 1:-1, :-2, 1:-1]
    total = total + padded[..., 1:-1, 1:-1, 2:] + padded[..., 1:-1, 1:-1, :-2]
    return total


def complex_times(first, second):
    return jnp.stack([first[0] * second[0] - first[1] * second[1], first[0] * second[1] + first[1] * second[0]])


def relax(spectrum, inverse):
    field = complex_times(inverse, spectrum)
    for repeat in range(SWEEPS - 1):
        field = complex_times(inverse, spectrum + coupling * neighbours(field))
    return field


def inverse_diagonal(angle, absorption, gamma):
    real_part = 1.0 - gamma * jnp.cos(angle) + absorption + 6.0 * coupling
    imag_part = jnp.broadcast_to(gamma * jnp.sin(angle), real_part.shape)
    magnitude = real_part * real_part + imag_part * imag_part
    return jnp.stack([real_part / magnitude, -imag_part / magnitude])


def reference(initial_state, source, absorption):
    gamma = alpha_corner ** (1.0 / STEPS)
    moments = jnp.arange(STEPS, dtype=jnp.float32)
    scale = (gamma ** moments)[None, :, None, None, None]
    angle = (moments * (2.0 * math.pi / STEPS))[:, None, None, None]
    inverse = inverse_diagonal(angle, absorption, gamma)[:, None]
    state = jnp.zeros_like(source)
    for repeat in range(ITERS):
        ends = state[:, -1]
        before = jnp.concatenate([initial_state[None], ends[:-1]], axis=0)
        forcing = source.at[:, 0].add(before - alpha_corner * ends)
        spectrum_full = jnp.fft.fft(forcing * scale, axis=1)
        field = relax(jnp.stack([spectrum_full.real, spectrum_full.imag]), inverse)
        state = jnp.fft.ifft(field[0] + 1j * field[1], axis=1).real / scale
    return state
```

```python
import functools
import math

import jax
import jax.numpy as jnp
from jax import lax
from jax.experimental import pallas as pl
from jax.experimental.pallas import tpu as pltpu
from jax.sharding import PartitionSpec as P

SWEEPS = 8
LANES = 128

alpha_corner = 0.1
coupling = 0.05

VMEM = pl.BlockSpec(memory_space=pltpu.VMEM)


REACH = SWEEPS - 1
HALO = 2 * REACH


def call(body, out_shape, *args, scratch=()):
    return pl.pallas_call(
        body,
        out_shape=out_shape,
        in_specs=[VMEM] * len(args),
        out_specs=jax.tree.map(lambda _: VMEM, out_shape),
        scratch_shapes=list(scratch),
        compiler_params=pltpu.CompilerParams(vmem_limit_bytes=48 * 1024 * 1024),
    )(*args)


def f32(*shape):
    return jax.ShapeDtypeStruct(shape, jnp.float32)


def rotate(value, turn):
    real, imag = value
    cosine, sine = math.cos(turn), math.sin(turn)
    if abs(sine) < 1e-12:
        return (real * cosine, imag * cosine if imag is not None else None)
    if imag is None:
        return (None if abs(cosine) < 1e-12 else real * cosine, real * sine)
    if abs(cosine) < 1e-12:
        return (imag * -sine, real * sine)
    return (real * cosine - imag * sine, real * sine + imag * cosine)


def plus(first, second, sign=1):
    def one(a, b):
        if b is None:
            return a
        if a is None:
            return b if sign == 1 else -b
        return a + b if sign == 1 else a - b

    return (one(first[0], second[0]), one(first[1], second[1]))


def conj(value):
    return (value[0], None if value[1] is None else -value[1])


def forward(values):
    size = len(values)
    if size == 1:
        return [(values[0], None)]
    even, odd = forward(values[0::2]), forward(values[1::2])
    half = size // 2
    result = [None] * (half + 1)
    for j in range(half // 2 + 1):
        turned = rotate(odd[j], -2.0 * math.pi * j / size)
        result[j] = plus(even[j], turned)
        result[half - j] = conj(plus(even[j], turned, -1))
    return result


def backward(spectrum, size):
    if size == 1:
        return [spectrum[0][0]]
    half = size // 2
    even, odd = [], []
    for j in range(half // 2 + 1):
        other = conj(spectrum[half - j])
        even.append(plus(spectrum[j], other))
        odd.append(rotate(plus(spectrum[j], other, -1), 2.0 * math.pi * j / size))
    for part in (even, odd):
        part[0] = (part[0][0], None)
        if half > 1:
            part[half // 2] = (part[half // 2][0], None)
    result = [None] * size
    result[0::2] = backward(even, half)
    result[1::2] = backward(odd, half)
    return result


def groups(window_len):
    table = [(0,)]
    for j in range(1, window_len // 2):
        table.append((2 * j - 1, 2 * j))
    table.append((window_len - 1,))
    return table


def pick(index, values):
    chosen = jnp.float32(values[0])
    for k in range(1, len(values)):
        chosen = jnp.where(index == k, jnp.float32(values[k]), chosen)
    return chosen


def planes_of(ref, scratch, pad, rows, load):
    depth = ref.shape[1]
    for r in range(rows):
        scratch[pl.ds(pad * rows + r, depth, stride=rows), :] = load(r).T


def pack_body(window_len, rows, source, initial, *refs):
    outs, scratch = refs[:-1], refs[-1]
    depth = source.shape[1]
    step = lax.axis_index("step")
    window = lax.axis_index("win")
    gamma = alpha_corner ** (1.0 / window_len)
    factor = pick(step, [gamma**t / coupling for t in range(window_len)])
    opening = jnp.where(jnp.logical_and(step == 0, window == 0), factor, 0.0)
    edge = jnp.zeros((HALO * rows, LANES), jnp.float32)
    scratch[: HALO * rows, :] = edge
    scratch[(HALO + depth) * rows :, :] = edge

    def load(r):
        cells = slice(r * LANES, (r + 1) * LANES)
        return source[cells, :] * factor + initial[cells, :] * opening

    planes_of(source, scratch, HALO, rows, load)
    pair = step // 2
    width = 2 * (depth // window_len)
    for d, out in enumerate(outs):
        start = pl.multiple_of((pair ^ d) * (width * rows), width * rows)
        out[...] = scratch[pl.ds(start, out.shape[0]), :]


def inverse_body(window_len, rows, absorption, coefs, scratch):
    depth = absorption.shape[1]
    step = lax.axis_index("step")
    gamma = alpha_corner ** (1.0 / window_len)
    planes_of(
        absorption,
        scratch,
        0,
        rows,
        lambda r: absorption[r * LANES : (r + 1) * LANES, :],
    )
    first = step * (depth // window_len) - HALO

    def one(i, carry):
        z = first + i
        inside = jnp.logical_and(z >= 0, z < depth)
        top = jnp.where(inside, jnp.float32(coupling), 0.0)
        start = pl.multiple_of(jnp.clip(z, 0, depth - 1) * rows, rows)
        cell = scratch[pl.ds(start, rows), :]
        for j, fields in enumerate(groups(window_len)):
            angle = 2.0 * math.pi * j / window_len
            real = cell + (1.0 - gamma * math.cos(angle) + 6.0 * coupling)
            if len(fields) == 1:
                coefs[fields[0], i] = top / real
            else:
                imag = gamma * math.sin(angle)
                ratio = top / (real * real + imag * imag)
                coefs[fields[0], i] = real * ratio
                coefs[fields[1], i] = ratio * -imag
        return carry

    lax.fori_loop(0, coefs.shape[1], one, 0, unroll=2)


def times(coefs, fields, i, values):
    first = coefs[fields[0], i]
    if len(fields) == 1:
        return (first * values[0],)
    second = coefs[fields[1], i]
    if values[1] is None:
        return (first * values[0], second * values[0])
    return (
        first * values[0] - second * values[1],
        first * values[1] + second * values[0],
    )


class Shifts:
    def __init__(self, rows, width):
        shape = (rows, LANES)
        lane = lax.broadcasted_iota(jnp.int32, shape, 1)
        row = lax.broadcasted_iota(jnp.int32, shape, 0)
        self.rows, self.width = rows, width
        self.low = lane % width != 0
        self.high = lane % width != width - 1
        self.opens = lane < width
        self.closes = lane >= LANES - width
        self.not_first = row != 0
        self.not_last = row != rows - 1

    def around(self, v):
        zero = jnp.zeros_like(v)
        total = jnp.where(self.low, pltpu.roll(v, 1, 1), zero)
        total = total + jnp.where(self.high, pltpu.roll(v, LANES - 1, 1), zero)
        down = jnp.where(self.not_first, pltpu.roll(v, 1, 0), zero)
        total = total + pltpu.roll(jnp.where(self.closes, down, v), self.width, 1)
        up = jnp.where(self.not_last, pltpu.roll(v, self.rows - 1, 0), zero)
        total = total + pltpu.roll(
            jnp.where(self.opens, up, v), LANES - self.width, 1
        )
        return total


def sweep(window_len, shifts, field, base, coefs, offset, low, high, finish):
    def one(i, carry):
        olds = []
        news = []
        for j, fields in enumerate(groups(window_len)):
            sums = []
            for k in fields:
                before, here = carry[k]
                after = field[k, i + 1]
                sums.append(shifts.around(here) + (before + after))
                olds.append((here, after))
            product = times(coefs, fields, i + offset, sums)
            news.append(tuple(base[k, i] + p for k, p in zip(fields, product)))
        finish(i, news)
        return tuple(olds)

    start = tuple((field[k, low - 1], field[k, low]) for k in range(window_len))
    lax.fori_loop(low, high, one, start, unroll=2)


def keep(window_len, field):
    def finish(i, news):
        for fields, parts in zip(groups(window_len), news):
            for k, value in zip(fields, parts):
                field[k, i] = value

    return finish


def first_body(window_len, width, mine, other, coefs, ends, base_out, field, base):
    count, rows = mine.shape[1], mine.shape[2]
    step = lax.axis_index("step")
    pair, is_even = step // 2, step % 2 == 0
    shifts = Shifts(rows, width)

    def transform(i, carry):
        values = []
        for c in range(window_len // 2):
            a, b = mine[pair ^ c, i], other[pair ^ c, i]
            values += [jnp.where(is_even, a, b), jnp.where(is_even, b, a)]
        for fields, value in zip(groups(window_len), forward(values)):
            for k, part in zip(fields, times(coefs, fields, i, value)):
                field[k, i] = part
                base[k, i] = part
        return carry

    lax.fori_loop(0, count, transform, 0, unroll=2)
    base_out[...] = base[:, REACH : count - REACH]

    gamma = alpha_corner ** (1.0 / window_len)
    last = window_len - 1
    share = 1.0 / (window_len * gamma**last)

    def to_ends(i, news):
        total = None
        for j, parts in enumerate(news):
            angle = 2.0 * math.pi * j * last / window_len
            both = share if len(parts) == 1 else 2.0 * share
            term = parts[0] * (both * math.cos(angle))
            if len(parts) == 2:
                term = term - parts[1] * (both * math.sin(angle))
            total = term if total is None else total + term
        ends[i - REACH] = total

    for k in range(1, SWEEPS):
        finish = to_ends if k == REACH else keep(window_len, field)
        sweep(window_len, shifts, field, base, coefs, 0, k, count - k, finish)


def second_body(window_len, width, base_in, coefs, ends, before, *refs):
    outs, (field, base, result) = refs[:-3], refs[-3:]
    count, rows = base_in.shape[1], base_in.shape[2]
    step = lax.axis_index("step")
    shifts = Shifts(rows, width)

    def correct(i, carry):
        change = (before[i] - alpha_corner * ends[i]) * (1.0 / coupling)
        for fields in groups(window_len):
            parts = times(coefs, fields, i + REACH, (change, None))
            for k, part in zip(fields, parts):
                value = base_in[k, i] + part
                field[k, i] = value
                base[k, i] = value
        return carry

    lax.fori_loop(0, count, correct, 0, unroll=2)

    def to_steps(i, news):
        spectrum = [parts if len(parts) == 2 else (parts[0], None) for parts in news]
        for t, value in enumerate(backward(spectrum, window_len)):
            result[t, i - REACH] = value

    for k in range(1, SWEEPS):
        finish = to_steps if k == REACH else keep(window_len, field)
        sweep(window_len, shifts, field, base, coefs, REACH, k, count - k, finish)
    for d, out in enumerate(outs):
        out[...] = result[step ^ d]


def unpack_body(window_len, rows, *refs):
    pieces, (out, scratch) = refs[:-2], refs[-2:]
    step = lax.axis_index("step")
    gamma = alpha_corner ** (1.0 / window_len)
    factor = pick(step, [1.0 / (window_len * gamma**t) for t in range(window_len)])
    length = pieces[0].shape[0]
    for d, piece in enumerate(pieces):
        start = pl.multiple_of((step ^ d) * length, length)
        scratch[pl.ds(start, length), :] = piece[...]
    depth = out.shape[1]
    for r in range(rows):
        block = scratch[pl.ds(r, depth, stride=rows), :]
        out[r * LANES : (r + 1) * LANES, :] = block.T * factor


def exchange(block, distance, count):
    return lax.ppermute(block, "step", [(i, i ^ distance) for i in range(count)])


def per_device(initial_state, source, absorption):
    window_len = lax.axis_size("step")
    windows = lax.axis_size("win")
    step = lax.axis_index("step")
    nx, ny, nz = absorption.shape
    cells = nx * ny
    rows = cells // LANES
    pairs = window_len // 2
    height = nz // window_len
    count = height + 2 * HALO
    pair_rows = (2 * height + 2 * HALO) * rows
    inner = height + 2 * REACH
    plane = (rows, LANES)

    packed = call(
        functools.partial(pack_body, window_len, rows),
        [f32(pair_rows, LANES)] * pairs,
        source.reshape(cells, nz),
        initial_state.reshape(cells, nz),
        scratch=[pltpu.VMEM(((nz + 2 * HALO) * rows, LANES), jnp.float32)],
    )
    received = [packed[0]]
    for d in range(1, pairs):
        received.append(exchange(packed[d], 2 * d, window_len))
    coefs = call(
        functools.partial(inverse_body, window_len, rows),
        f32(window_len, count, *plane),
        absorption.reshape(cells, nz),
        scratch=[pltpu.VMEM((nz * rows, LANES), jnp.float32)],
    )
    both = jnp.stack(received).reshape(pairs, 2 * height + 2 * HALO, *plane)
    core = step % 2
    mine = lax.dynamic_slice_in_dim(both, core * height, count, 1)
    other = lax.dynamic_slice_in_dim(both, (1 - core) * height, count, 1)
    other = exchange(other, 1, window_len)

    ends, base = call(
        functools.partial(first_body, window_len, ny),
        [f32(inner, *plane), f32(window_len, inner, *plane)],
        mine,
        other,
        coefs,
        scratch=[pltpu.VMEM((window_len, count, *plane), jnp.float32)] * 2,
    )
    before = lax.ppermute(ends, "win", [(w - 1, w) for w in range(1, windows)])
    results = call(
        functools.partial(second_body, window_len, ny),
        [f32(height, *plane)] * window_len,
        base,
        coefs,
        ends,
        before,
        scratch=[pltpu.VMEM((window_len, inner, *plane), jnp.float32)] * 2
        + [pltpu.VMEM((window_len, height, *plane), jnp.float32)],
    )
    order = sorted(range(1, window_len), key=lambda d: -bin(d // 2).count("1"))
    pieces = [results[0]] + [None] * (window_len - 1)
    for d in order:
        pieces[d] = exchange(results[d], d, window_len)
    state = call(
        functools.partial(unpack_body, window_len, rows),
        f32(cells, nz),
        *[p.reshape(height * rows, LANES) for p in pieces],
        scratch=[pltpu.VMEM((nz * rows, LANES), jnp.float32)],
    )
    return state.reshape(1, 1, nx, ny, nz)


def solution(mesh):
    return jax.shard_map(
        per_device,
        mesh=mesh,
        in_specs=(P(), P("win", "step", None, None, None), P()),
        out_specs=P("win", "step", None, None, None),
        check_vma=False,
    )
```

```python
import functools
import math

import jax
import jax.numpy as jnp
from jax import lax
from jax.experimental import pallas as pl
from jax.experimental.pallas import tpu as pltpu
from jax.sharding import PartitionSpec as P

SWEEPS = 8
LANES = 128

alpha_corner = 0.1
coupling = 0.05

VMEM = pl.BlockSpec(memory_space=pltpu.VMEM)


REACH = SWEEPS - 1
HALO = 2 * REACH


def call(body, out_shape, *args, scratch=()):
    return pl.pallas_call(
        body,
        out_shape=out_shape,
        in_specs=[VMEM] * len(args),
        out_specs=jax.tree.map(lambda _: VMEM, out_shape),
        scratch_shapes=list(scratch),
        compiler_params=pltpu.CompilerParams(vmem_limit_bytes=48 * 1024 * 1024),
    )(*args)


def f32(*shape):
    return jax.ShapeDtypeStruct(shape, jnp.float32)


def rotate(value, turn):
    real, imag = value
    cosine, sine = math.cos(turn), math.sin(turn)
    if abs(sine) < 1e-12:
        return (real * cosine, imag * cosine if imag is not None else None)
    if imag is None:
        return (None if abs(cosine) < 1e-12 else real * cosine, real * sine)
    if abs(cosine) < 1e-12:
        return (imag * -sine, real * sine)
    return (real * cosine - imag * sine, real * sine + imag * cosine)


def plus(first, second, sign=1):
    def one(a, b):
        if b is None:
            return a
        if a is None:
            return b if sign == 1 else -b
        return a + b if sign == 1 else a - b

    return (one(first[0], second[0]), one(first[1], second[1]))


def conj(value):
    return (value[0], None if value[1] is None else -value[1])


def forward(values):
    size = len(values)
    if size == 1:
        return [(values[0], None)]
    even, odd = forward(values[0::2]), forward(values[1::2])
    half = size // 2
    result = [None] * (half + 1)
    for j in range(half // 2 + 1):
        turned = rotate(odd[j], -2.0 * math.pi * j / size)
        result[j] = plus(even[j], turned)
        result[half - j] = conj(plus(even[j], turned, -1))
    return result


def backward(spectrum, size):
    if size == 1:
        return [spectrum[0][0]]
    half = size // 2
    even, odd = [], []
    for j in range(half // 2 + 1):
        other = conj(spectrum[half - j])
        even.append(plus(spectrum[j], other))
        odd.append(rotate(plus(spectrum[j], other, -1), 2.0 * math.pi * j / size))
    for part in (even, odd):
        part[0] = (part[0][0], None)
        if half > 1:
            part[half // 2] = (part[half // 2][0], None)
    result = [None] * size
    result[0::2] = backward(even, half)
    result[1::2] = backward(odd, half)
    return result


class Plane:
    def __init__(self, nx, ny):
        self.rows = nx * ny // LANES
        self.by = 2 if self.rows % 2 == 0 and ny % 2 == 0 else 1
        self.bx = self.rows // self.by
        self.qy = ny // self.by
        self.qx = nx // self.bx
        assert self.qx * self.qy == LANES

    def cells(self, row):
        first, second = row // self.by, row % self.by
        for q in range(self.qx):
            yield q, q * self.bx + first, pl.ds(second, self.qy, stride=self.by)

    def read(self, ref, row):
        return jnp.concatenate([ref[x, y, :] for _, x, y in self.cells(row)], axis=0)

    def write(self, ref, row, value):
        for q, x, y in self.cells(row):
            ref[x, y, :] = value[q * self.qy : (q + 1) * self.qy]


def pick(index, values):
    chosen = jnp.float32(values[0])
    for k in range(1, len(values)):
        chosen = jnp.where(index == k, jnp.float32(values[k]), chosen)
    return chosen


def pack_body(window_len, plane, source, initial, *refs):
    outs, scratch = refs[:-1], refs[-1]
    rows, depth = plane.rows, source.shape[2]
    step = lax.axis_index("step")
    window = lax.axis_index("win")
    gamma = alpha_corner ** (1.0 / window_len)
    factor = pick(step, [gamma**t / coupling for t in range(window_len)])
    opening = jnp.where(jnp.logical_and(step == 0, window == 0), factor, 0.0)
    edge = jnp.zeros((HALO * rows, LANES), jnp.float32)
    scratch[: HALO * rows, :] = edge
    scratch[(HALO + depth) * rows :, :] = edge
    for r in range(rows):
        block = plane.read(source, r) * factor + plane.read(initial, r) * opening
        scratch[pl.ds(HALO * rows + r, depth, stride=rows), :] = block.T
    pair = step // 2
    width = 2 * (depth // window_len)
    for d, out in enumerate(outs):
        start = pl.multiple_of((pair ^ d) * (width * rows), width * rows)
        out[...] = scratch[pl.ds(start, out.shape[0]), :]


def inverse_body(window_len, plane, absorption, coefs, same, cross, scratch):
    rows, depth, half = plane.rows, absorption.shape[2], window_len // 2
    step = lax.axis_index("step")
    gamma = alpha_corner ** (1.0 / window_len)
    for r in range(rows):
        scratch[pl.ds(r, depth, stride=rows), :] = plane.read(absorption, r).T
    first = step * (depth // window_len) - HALO

    def one(i, carry):
        z = first + i
        inside = jnp.logical_and(z >= 0, z < depth)
        top = jnp.where(inside, jnp.float32(coupling), 0.0)
        start = pl.multiple_of(jnp.clip(z, 0, depth - 1) * rows, rows)
        cell = scratch[pl.ds(start, rows), :]
        origin = pl.multiple_of(i * (rows * window_len), rows * window_len)

        def spread(ref, k, value):
            ref[pl.ds(origin + k, rows, stride=window_len), :] = value

        for j in range(half + 1):
            angle = 2.0 * math.pi * j / window_len
            real = cell + (1.0 - gamma * math.cos(angle) + 6.0 * coupling)
            if j in (0, half):
                value = top / real
                coefs[j, i] = value
                spread(same, j, value)
                spread(cross, j, jnp.zeros_like(value))
                continue
            imag = gamma * math.sin(angle)
            ratio = top / (real * real + imag * imag)
            first_part, second_part = real * ratio, ratio * -imag
            coefs[j, i] = first_part
            coefs[half + j, i] = second_part
            spread(same, j, first_part)
            spread(same, half + j, first_part)
            spread(cross, j, -second_part)
            spread(cross, half + j, second_part)
        return carry

    lax.fori_loop(0, coefs.shape[1], one, 0, unroll=2)


class Field:
    def __init__(self, ref, window_len, rows):
        self.ref, self.n, self.rows = ref, window_len, rows

    def span(self, i, r):
        return pl.ds((i * self.rows + r) * self.n, self.n)

    def get(self, i, r):
        return self.ref[self.span(i, r), :]

    def put(self, i, r, value):
        self.ref[self.span(i, r), :] = value

    def part(self, i, k):
        return pl.ds(i * (self.rows * self.n) + k, self.rows, stride=self.n)

    def get_part(self, i, k):
        return self.ref[self.part(i, k), :]

    def put_part(self, i, k, value):
        self.ref[self.part(i, k), :] = value

    def plane(self, i):
        return [self.get(i, r) for r in range(self.rows)]


class Sweeps:
    def __init__(self, window_len, plane):
        self.n, self.grid = window_len, plane
        lane = lax.broadcasted_iota(jnp.int32, (window_len, LANES), 1)
        self.y_low = lane % plane.qy != 0
        self.y_high = lane % plane.qy != plane.qy - 1
        self.x_low = lane >= plane.qy
        self.x_high = lane < LANES - plane.qy

    def around(self, here):
        grid = self.grid
        bx, by = grid.bx, grid.by

        def moved(r, amount, inside):
            return jnp.where(inside, pltpu.roll(here[r], amount % LANES, 1), 0.0)

        sums = []
        for r in range(grid.rows):
            x, y = r // by, r % by
            if x > 0:
                west = here[r - by]
            else:
                west = moved(r + (bx - 1) * by, grid.qy, self.x_low)
            if x < bx - 1:
                east = here[r + by]
            else:
                east = moved(r - (bx - 1) * by, -grid.qy, self.x_high)
            south = here[r - 1] if y > 0 else moved(r + by - 1, 1, self.y_low)
            north = here[r + 1] if y < by - 1 else moved(r - by + 1, -1, self.y_high)
            sums.append((west + east) + (south + north))
        return sums

    def run(self, source, target, base, shift, same, cross, offset, low, high, lead):
        before, here = source.plane(low - 1), source.plane(low)
        for i in range(low, high):
            after = source.plane(i + 1)
            sums = self.around(here)
            for r in range(self.grid.rows):
                total = sums[r] + (before[r] + after[r])
                turned = pltpu.roll(total, self.n // 2, 0)
                value = same.get(i + offset, r) * total
                value = value + cross.get(i + offset, r) * turned
                target.put(i - lead, r, base.get(i + shift, r) + value)
            before, here = here, after

    def all(self, field, final, base, shift, same, cross, offset, count):
        for k in range(1, SWEEPS):
            source = base if k == 1 else field
            target, lead = (final, REACH) if k == REACH else (field, 0)
            self.run(
                source, target, base, shift, same, cross, offset, k, count - k, lead
            )


def first_body(
    window_len, plane, mine, other, coefs, same, cross, ends, base_ref, field_ref, tail
):
    count, half = mine.shape[1], window_len // 2
    step = lax.axis_index("step")
    pair, is_even = step // 2, step % 2 == 0
    wrap = functools.partial(Field, window_len=window_len, rows=plane.rows)
    base, final = wrap(base_ref), wrap(tail)

    for i in range(count):
        values = []
        for c in range(half):
            a, b = mine[pair ^ c, i], other[pair ^ c, i]
            values += [jnp.where(is_even, a, b), jnp.where(is_even, b, a)]
        for j, (real, imag) in enumerate(forward(values)):
            first = coefs[j, i]
            if j in (0, half):
                base.put_part(i, j, first * real)
                continue
            second = coefs[half + j, i]
            base.put_part(i, j, first * real - second * imag)
            base.put_part(i, half + j, first * imag + second * real)

    Sweeps(window_len, plane).all(
        wrap(field_ref), final, base, 0, wrap(same), wrap(cross), 0, count
    )
    gamma = alpha_corner ** (1.0 / window_len)
    last = window_len - 1
    share = 1.0 / (window_len * gamma**last)
    for i in range(count - 2 * REACH):
        total = None
        for j in range(half + 1):
            angle = 2.0 * math.pi * j * last / window_len
            both = share if j in (0, half) else 2.0 * share
            term = final.get_part(i, j) * (both * math.cos(angle))
            if j not in (0, half):
                term = term - final.get_part(i, half + j) * (both * math.sin(angle))
            total = term if total is None else total + term
        ends[i] = total


def second_body(window_len, plane, base_in, same, cross, ends, before, *refs):
    outs, (change, field_ref, base_ref, tail) = refs[:-4], refs[-4:]
    count, rows, half = ends.shape[0], plane.rows, window_len // 2
    step = lax.axis_index("step")
    wrap = functools.partial(Field, window_len=window_len, rows=rows)
    old, base, final = wrap(base_in), wrap(base_ref), wrap(tail)
    same, cross = wrap(same), wrap(cross)
    block = lax.broadcasted_iota(jnp.int32, (window_len, LANES), 0)
    is_real = block <= half

    for i in range(count):
        change[i] = (before[i] - alpha_corner * ends[i]) * (1.0 / coupling)
    for i in range(count):
        for r in range(rows):
            step_in = jnp.broadcast_to(change[i, r : r + 1, :], (window_len, LANES))
            at = i + REACH
            weight = jnp.where(is_real, same.get(at, r), cross.get(at, r))
            base.put(i, r, old.get(at, r) + weight * step_in)

    Sweeps(window_len, plane).all(
        wrap(field_ref), final, base, 0, same, cross, REACH, count
    )
    for i in range(count - 2 * REACH):
        spectrum = []
        for j in range(half + 1):
            imag = None if j in (0, half) else final.get_part(i, half + j)
            spectrum.append((final.get_part(i, j), imag))
        for t, value in enumerate(backward(spectrum, window_len)):
            field_ref[pl.ds((t * (count - 2 * REACH) + i) * rows, rows), :] = value
    size = (count - 2 * REACH) * rows
    for d, out in enumerate(outs):
        out[...] = field_ref[pl.ds(pl.multiple_of((step ^ d) * size, size), size), :]


def unpack_body(window_len, plane, *refs):
    pieces, (out, scratch) = refs[:-2], refs[-2:]
    step = lax.axis_index("step")
    gamma = alpha_corner ** (1.0 / window_len)
    factor = pick(step, [1.0 / (window_len * gamma**t) for t in range(window_len)])
    length = pieces[0].shape[0]
    for d, piece in enumerate(pieces):
        start = pl.multiple_of((step ^ d) * length, length)
        scratch[pl.ds(start, length), :] = piece[...]
    for r in range(plane.rows):
        block = scratch[pl.ds(r, out.shape[2], stride=plane.rows), :]
        plane.write(out, r, block.T * factor)


def exchange(block, distance, count):
    return lax.ppermute(block, "step", [(i, i ^ distance) for i in range(count)])


def per_device(initial_state, source, absorption):
    window_len = lax.axis_size("step")
    windows = lax.axis_size("win")
    core = lax.axis_index("step") % 2
    nx, ny, nz = absorption.shape
    plane = Plane(nx, ny)
    rows = plane.rows
    pairs = window_len // 2
    height = nz // window_len
    count = height + 2 * HALO
    wide = 2 * height + 2 * HALO
    inner = height + 2 * REACH
    block = rows * window_len

    def space(*shape):
        return pltpu.VMEM(shape, jnp.float32)

    packed = call(
        functools.partial(pack_body, window_len, plane),
        [f32(wide * rows, LANES)] * pairs,
        source[0, 0],
        initial_state,
        scratch=[space((nz + 2 * HALO) * rows, LANES)],
    )
    received = [packed[0]]
    for d in range(1, pairs):
        received.append(exchange(packed[d], 2 * d, window_len))
    coefs, same, cross = call(
        functools.partial(inverse_body, window_len, plane),
        [f32(window_len, count, rows, LANES)] + [f32(count * block, LANES)] * 2,
        absorption,
        scratch=[space(nz * rows, LANES)],
    )
    both = jnp.stack(received).reshape(pairs, wide, rows, LANES)
    mine = lax.dynamic_slice_in_dim(both, core * height, count, 1)
    other = lax.dynamic_slice_in_dim(both, (1 - core) * height, count, 1)
    other = exchange(other, 1, window_len)

    ends, base = call(
        functools.partial(first_body, window_len, plane),
        [f32(inner, rows, LANES), f32(count * block, LANES)],
        mine,
        other,
        coefs,
        same,
        cross,
        scratch=[space(count * block, LANES), space(inner * block, LANES)],
    )
    before = lax.ppermute(ends, "win", [(w - 1, w) for w in range(1, windows)])
    results = call(
        functools.partial(second_body, window_len, plane),
        [f32(height * rows, LANES)] * window_len,
        base,
        same,
        cross,
        ends,
        before,
        scratch=[space(inner, rows, LANES)]
        + [space(inner * block, LANES)] * 2
        + [space(height * block, LANES)],
    )
    pieces = [results[0]] + [None] * (window_len - 1)
    for d in sorted(range(1, window_len), key=lambda d: -bin(d // 2).count("1")):
        pieces[d] = exchange(results[d], d, window_len)
    state = call(
        functools.partial(unpack_body, window_len, plane),
        f32(nx, ny, nz),
        *pieces,
        scratch=[space(nz * rows, LANES)],
    )
    return state[None, None]


def solution(mesh):
    return jax.shard_map(
        per_device,
        mesh=mesh,
        in_specs=(P(), P("win", "step", None, None, None), P()),
        out_specs=P("win", "step", None, None, None),
        check_vma=False,
    )
```

```python
import functools
import math

import jax
import jax.numpy as jnp
from jax import lax
from jax.experimental import pallas as pl
from jax.experimental.pallas import tpu as pltpu
from jax.sharding import PartitionSpec as P


SWEEPS = 8
LANES = 128

alpha_corner = 0.1
coupling = 0.05

VMEM = pl.BlockSpec(memory_space=pltpu.VMEM)


REACH = SWEEPS - 1
HALO = 2 * REACH


def call(body, out_shape, *args, scratch=()):
    return pl.pallas_call(
        body,
        out_shape=out_shape,
        in_specs=[VMEM] * len(args),
        out_specs=jax.tree.map(lambda _: VMEM, out_shape),
        scratch_shapes=list(scratch),
        compiler_params=pltpu.CompilerParams(vmem_limit_bytes=12 * 1024 * 1024),
    )(*args)


def f32(*shape):
    return jax.ShapeDtypeStruct(shape, jnp.float32)


def rotate(value, turn):
    real, imag = value
    cosine, sine = math.cos(turn), math.sin(turn)
    if abs(sine) < 1e-12:
        return (real * cosine, imag * cosine if imag is not None else None)
    if imag is None:
        return (None if abs(cosine) < 1e-12 else real * cosine, real * sine)
    if abs(cosine) < 1e-12:
        return (imag * -sine, real * sine)
    return (real * cosine - imag * sine, real * sine + imag * cosine)


def plus(first, second, sign=1):
    def one(a, b):
        if b is None:
            return a
        if a is None:
            return b if sign == 1 else -b
        return a + b if sign == 1 else a - b

    return (one(first[0], second[0]), one(first[1], second[1]))


def conj(value):
    return (value[0], None if value[1] is None else -value[1])


def forward(values):
    size = len(values)
    if size == 1:
        return [(values[0], None)]
    even, odd = forward(values[0::2]), forward(values[1::2])
    half = size // 2
    result = [None] * (half + 1)
    for j in range(half // 2 + 1):
        turned = rotate(odd[j], -2.0 * math.pi * j / size)
        result[j] = plus(even[j], turned)
        result[half - j] = conj(plus(even[j], turned, -1))
    return result


def backward(spectrum, size):
    if size == 1:
        return [spectrum[0][0]]
    half = size // 2
    even, odd = [], []
    for j in range(half // 2 + 1):
        other = conj(spectrum[half - j])
        even.append(plus(spectrum[j], other))
        odd.append(rotate(plus(spectrum[j], other, -1), 2.0 * math.pi * j / size))
    for part in (even, odd):
        part[0] = (part[0][0], None)
        if half > 1:
            part[half // 2] = (part[half // 2][0], None)
    result = [None] * size
    result[0::2] = backward(even, half)
    result[1::2] = backward(odd, half)
    return result


class Plane:
    def __init__(self, nx, ny):
        self.rows = nx * ny // LANES
        self.by = 2 if self.rows % 2 == 0 and ny % 2 == 0 else 1
        self.bx = self.rows // self.by
        self.qy = ny // self.by
        self.qx = nx // self.bx
        assert self.qx * self.qy == LANES

    def cells(self, row):
        first, second = row // self.by, row % self.by
        for q in range(self.qx):
            yield q, q * self.bx + first, pl.ds(second, self.qy, stride=self.by)

    def read(self, ref, row):
        return jnp.concatenate([ref[x, y, :] for _, x, y in self.cells(row)], axis=0)

    def write(self, ref, row, value):
        for q, x, y in self.cells(row):
            ref[x, y, :] = value[q * self.qy : (q + 1) * self.qy]


def pick(index, values):
    chosen = jnp.float32(values[0])
    for k in range(1, len(values)):
        chosen = jnp.where(index == k, jnp.float32(values[k]), chosen)
    return chosen


def pack_body(window_len, plane, source, *refs):
    outs, scratch = refs[:-1], refs[-1]
    rows, depth = plane.rows, source.shape[2]
    step = lax.axis_index("step")
    gamma = alpha_corner ** (1.0 / window_len)
    factor = pick(step, [gamma**t / coupling for t in range(window_len)])
    edge = jnp.zeros((HALO * rows, LANES), jnp.float32)
    scratch[: HALO * rows, :] = edge
    scratch[(HALO + depth) * rows :, :] = edge
    for r in range(rows):
        block = plane.read(source, r) * factor
        scratch[pl.ds(HALO * rows + r, depth, stride=rows), :] = block.T
    pair = step // 2
    width = 2 * (depth // window_len)
    for d, out in enumerate(outs):
        start = pl.multiple_of((pair ^ d) * (width * rows), width * rows)
        out[...] = scratch[pl.ds(start, out.shape[0]), :]


def local_body(
    window_len, plane, absorption, initial, coefs, same, cross, opening, *scratch
):
    rows, depth, half = plane.rows, absorption.shape[2], window_len // 2
    step = lax.axis_index("step")
    gamma = alpha_corner ** (1.0 / window_len)
    weight = jnp.where(lax.axis_index("win") == 0, jnp.float32(1.0 / coupling), 0.0)
    for r in range(rows):
        at = pl.ds(r, depth, stride=rows)
        scratch[0][at, :] = plane.read(absorption, r).T
        scratch[1][at, :] = (plane.read(initial, r) * weight).T
    first = step * (depth // window_len) - HALO

    def one(i, carry):
        z = first + i
        inside = jnp.logical_and(z >= 0, z < depth)
        top = jnp.where(inside, jnp.float32(coupling), 0.0)
        start = pl.multiple_of(jnp.clip(z, 0, depth - 1) * rows, rows)
        cell = scratch[0][pl.ds(start, rows), :]
        opening[i] = scratch[1][pl.ds(start, rows), :]
        origin = pl.multiple_of(i * (rows * window_len), rows * window_len)

        def spread(ref, k, value):
            ref[pl.ds(origin + k, rows, stride=window_len), :] = value

        for j in range(half + 1):
            angle = 2.0 * math.pi * j / window_len
            real = cell + (1.0 - gamma * math.cos(angle) + 6.0 * coupling)
            if j in (0, half):
                value = top / real
                coefs[j, i] = value
                spread(same, j, value)
                spread(cross, j, jnp.zeros_like(value))
                continue
            imag = gamma * math.sin(angle)
            ratio = top / (real * real + imag * imag)
            first_part, second_part = real * ratio, ratio * -imag
            coefs[j, i] = first_part
            coefs[half + j, i] = second_part
            spread(same, j, first_part)
            spread(same, half + j, first_part)
            spread(cross, j, -second_part)
            spread(cross, half + j, second_part)
        return carry

    lax.fori_loop(0, coefs.shape[1], one, 0, unroll=2)


class Field:
    def __init__(self, ref, window_len, rows):
        self.ref, self.n, self.rows = ref, window_len, rows

    def span(self, i, r):
        return pl.ds((i * self.rows + r) * self.n, self.n)

    def get(self, i, r):
        return self.ref[self.span(i, r), :]

    def put(self, i, r, value):
        self.ref[self.span(i, r), :] = value

    def part(self, i, k):
        return pl.ds(i * (self.rows * self.n) + k, self.rows, stride=self.n)

    def get_part(self, i, k):
        return self.ref[self.part(i, k), :]

    def put_part(self, i, k, value):
        self.ref[self.part(i, k), :] = value

    def plane(self, i):
        return [self.get(i, r) for r in range(self.rows)]


class Sweeps:
    def __init__(self, window_len, plane):
        self.n, self.grid = window_len, plane
        lane = lax.broadcasted_iota(jnp.int32, (window_len, LANES), 1)
        self.y_low = lane % plane.qy != 0
        self.y_high = lane % plane.qy != plane.qy - 1
        self.x_low = lane >= plane.qy
        self.x_high = lane < LANES - plane.qy

    def around(self, here):
        grid = self.grid
        bx, by = grid.bx, grid.by

        def moved(r, amount, inside):
            return jnp.where(inside, pltpu.roll(here[r], amount % LANES, 1), 0.0)

        sums = []
        for r in range(grid.rows):
            x, y = r // by, r % by
            if x > 0:
                west = here[r - by]
            else:
                west = moved(r + (bx - 1) * by, grid.qy, self.x_low)
            if x < bx - 1:
                east = here[r + by]
            else:
                east = moved(r - (bx - 1) * by, -grid.qy, self.x_high)
            south = here[r - 1] if y > 0 else moved(r + by - 1, 1, self.y_low)
            north = here[r + 1] if y < by - 1 else moved(r - by + 1, -1, self.y_high)
            sums.append((west + east) + (south + north))
        return sums

    def run(self, source, target, base, shift, same, cross, offset, low, high, lead):
        before, here = source.plane(low - 1), source.plane(low)
        for i in range(low, high):
            after = source.plane(i + 1)
            sums = self.around(here)
            for r in range(self.grid.rows):
                total = sums[r] + (before[r] + after[r])
                turned = pltpu.roll(total, self.n // 2, 0)
                value = same.get(i + offset, r) * total
                value = value + cross.get(i + offset, r) * turned
                target.put(i - lead, r, base.get(i + shift, r) + value)
            before, here = here, after

    def all(self, field, final, base, shift, same, cross, offset, count):
        for k in range(1, SWEEPS):
            source = base if k == 1 else field
            target, lead = (final, REACH) if k == REACH else (field, 0)
            self.run(
                source, target, base, shift, same, cross, offset, k, count - k, lead
            )


def first_body(
    window_len, plane, mine, other, coefs, same, cross, opening, ends, base_ref, *space
):
    field_ref, tail = space
    rows, half = plane.rows, window_len // 2
    count = other.shape[1] // rows
    height = mine.shape[1] // rows - count
    step = lax.axis_index("step")
    pair, is_even = step // 2, step % 2 == 0
    first_row = pl.multiple_of((step % 2) * (height * rows), height * rows)
    wrap = functools.partial(Field, window_len=window_len, rows=plane.rows)
    base, final = wrap(base_ref), wrap(tail)

    for i in range(count):
        values = []
        for c in range(half):
            a = mine[pair ^ c, pl.ds(first_row + i * rows, rows), :]
            b = other[pair ^ c, i * rows : (i + 1) * rows, :]
            values += [jnp.where(is_even, a, b), jnp.where(is_even, b, a)]
        for j, (real, imag) in enumerate(forward(values)):
            first = coefs[j, i]
            real = real + opening[i]
            if j in (0, half):
                base.put_part(i, j, first * real)
                continue
            second = coefs[half + j, i]
            base.put_part(i, j, first * real - second * imag)
            base.put_part(i, half + j, first * imag + second * real)

    Sweeps(window_len, plane).all(
        wrap(field_ref), final, base, 0, wrap(same), wrap(cross), 0, count
    )
    gamma = alpha_corner ** (1.0 / window_len)
    last = window_len - 1
    share = 1.0 / (window_len * gamma**last)
    for i in range(count - 2 * REACH):
        total = None
        for j in range(half + 1):
            angle = 2.0 * math.pi * j * last / window_len
            both = share if j in (0, half) else 2.0 * share
            term = final.get_part(i, j) * (both * math.cos(angle))
            if j not in (0, half):
                term = term - final.get_part(i, half + j) * (both * math.sin(angle))
            total = term if total is None else total + term
        ends[i] = total


def second_body(window_len, plane, base_in, same, cross, ends, before, *refs):
    outs, (change, field_ref, base_ref, tail) = refs[:-4], refs[-4:]
    count, rows, half = ends.shape[0], plane.rows, window_len // 2
    step = lax.axis_index("step")
    wrap = functools.partial(Field, window_len=window_len, rows=rows)
    old, base, final = wrap(base_in), wrap(base_ref), wrap(tail)
    same, cross = wrap(same), wrap(cross)
    block = lax.broadcasted_iota(jnp.int32, (window_len, LANES), 0)
    is_real = block <= half

    for i in range(count):
        change[i] = (before[i] - alpha_corner * ends[i]) * (1.0 / coupling)
    for i in range(count):
        for r in range(rows):
            step_in = jnp.broadcast_to(change[i, r : r + 1, :], (window_len, LANES))
            at = i + REACH
            weight = jnp.where(is_real, same.get(at, r), cross.get(at, r))
            base.put(i, r, old.get(at, r) + weight * step_in)

    Sweeps(window_len, plane).all(
        wrap(field_ref), final, base, 0, same, cross, REACH, count
    )
    for i in range(count - 2 * REACH):
        spectrum = []
        for j in range(half + 1):
            imag = None if j in (0, half) else final.get_part(i, half + j)
            spectrum.append((final.get_part(i, j), imag))
        for t, value in enumerate(backward(spectrum, window_len)):
            field_ref[pl.ds((t * (count - 2 * REACH) + i) * rows, rows), :] = value
    size = (count - 2 * REACH) * rows
    for d, out in enumerate(outs):
        out[...] = field_ref[pl.ds(pl.multiple_of((step ^ d) * size, size), size), :]


def unpack_body(window_len, plane, *refs):
    pieces, (out, scratch) = refs[:-2], refs[-2:]
    step = lax.axis_index("step")
    gamma = alpha_corner ** (1.0 / window_len)
    factor = pick(step, [1.0 / (window_len * gamma**t) for t in range(window_len)])
    length = pieces[0].shape[0]
    for d, piece in enumerate(pieces):
        start = pl.multiple_of((step ^ d) * length, length)
        scratch[pl.ds(start, length), :] = piece[...]
    for r in range(plane.rows):
        block = scratch[pl.ds(r, out.shape[2], stride=plane.rows), :]
        plane.write(out, r, block.T * factor)


def exchange(block, distance, count):
    return lax.ppermute(block, "step", [(i, i ^ distance) for i in range(count)])


def per_device(initial_state, source, absorption):
    window_len = lax.axis_size("step")
    windows = lax.axis_size("win")
    core = lax.axis_index("step") % 2
    nx, ny, nz = absorption.shape
    plane = Plane(nx, ny)
    rows = plane.rows
    pairs = window_len // 2
    height = nz // window_len
    count = height + 2 * HALO
    wide = 2 * height + 2 * HALO
    inner = height + 2 * REACH
    block = rows * window_len

    def space(*shape):
        return pltpu.VMEM(shape, jnp.float32)

    packed = call(
        functools.partial(pack_body, window_len, plane),
        [f32(wide * rows, LANES)] * pairs,
        source[0, 0],
        scratch=[space((nz + 2 * HALO) * rows, LANES)],
    )
    received = [packed[0]] + [None] * (pairs - 1)
    for d in range(1, pairs):
        received[d] = exchange(packed[d], 2 * d, window_len)
    coefs, same, cross, opening = call(
        functools.partial(local_body, window_len, plane),
        [f32(window_len, count, rows, LANES)]
        + [f32(count * block, LANES)] * 2
        + [f32(count, rows, LANES)],
        absorption,
        initial_state,
        scratch=[space(nz * rows, LANES)] * 2,
    )
    mine = jnp.stack(received)
    start = (1 - core) * (height * rows)
    other = jnp.stack(
        [
            exchange(
                lax.dynamic_slice_in_dim(piece, start, count * rows), 1, window_len
            )
            for piece in received
        ]
    )

    ends, base = call(
        functools.partial(first_body, window_len, plane),
        [f32(inner, rows, LANES), f32(count * block, LANES)],
        mine,
        other,
        coefs,
        same,
        cross,
        opening,
        scratch=[space(count * block, LANES), space(inner * block, LANES)],
    )
    before = lax.ppermute(ends, "win", [(w - 1, w) for w in range(1, windows)])
    results = call(
        functools.partial(second_body, window_len, plane),
        [f32(height * rows, LANES)] * window_len,
        base,
        same,
        cross,
        ends,
        before,
        scratch=[space(inner, rows, LANES)]
        + [space(inner * block, LANES)] * 2
        + [space(height * block, LANES)],
    )
    pieces = [results[0]] + [None] * (window_len - 1)
    for d in sorted(range(1, window_len), key=lambda d: -bin(d // 2).count("1")):
        pieces[d] = exchange(results[d], d, window_len)
    state = call(
        functools.partial(unpack_body, window_len, plane),
        f32(nx, ny, nz),
        *pieces,
        scratch=[space(nz * rows, LANES)],
    )
    return state[None, None]


def solution(mesh):
    return jax.shard_map(
        per_device,
        mesh=mesh,
        in_specs=(P(), P("win", "step", None, None, None), P()),
        out_specs=P("win", "step", None, None, None),
        check_vma=False,
    )
```
